8 devices in a mesh: dp: 1 (over z), pz: 2 (over y), py: 2 (over x), px: 2 (over core).
Axes of the slice: x: 2, y: 2, z: 1, core: 2. Of those that a mesh axis runs over, the one named last changes fastest.
Arguments:
- volumes: bfloat16 [2, 32, 128, 128, 128], P('dp', None, 'px', 'py', 'pz')
- filter_taps: float32 [3, 3, 25], replicated
- mix_weight: bfloat16 [3, 32, 32], replicated
- mix_bias: float32 [3, 32], replicated
Outputs:
- output: bfloat16 [2, 32, 128, 128, 128], P('dp', None, 'px', 'py', 'pz')
All inputs are finite; a program needn't handle non-finite values.
Results may differ from the reference program's by a relative error of at most 0.00543444.
Values are sent between devices in bfloat16 or wider.
A program may use at most 1 GiB of HBM per device.

```python
import jax
import jax.numpy as jnp
from jax import lax

CHANNELS = 32
TAPS = 25
LAYERS = 3
VOLUMES = 2
EXTENT_X = 128
EXTENT_Y = 128
EXTENT_Z = 128
HALF_WIDTH = (TAPS - 1) // 2


def setup_inputs(seed: int = 0, part: int = 0) -> dict:
    root_key = jax.random.key(seed)
    key_vol, key_sign, key_mag, key_mix, key_bias = jax.random.split(root_key, 5)
    vol_key = jax.random.fold_in(key_vol, part)
    volumes = jax.random.normal(vol_key, (VOLUMES, CHANNELS, EXTENT_X, EXTENT_Y, EXTENT_Z), jnp.float32).astype(jnp.bfloat16)
    tap_signs = jax.random.bernoulli(key_sign, 0.5, (LAYERS, 3, TAPS)).astype(jnp.float32) * 2.0 - 1.0
    tap_sizes = jax.random.uniform(key_mag, (LAYERS, 3, TAPS), jnp.float32, 0.5, 1.5)
    raw_taps = tap_signs * tap_sizes
    filter_taps = raw_taps / jnp.sqrt(jnp.sum(raw_taps * raw_taps, axis=-1, keepdims=True))
    mix_weight = (jax.random.normal(key_mix, (LAYERS, CHANNELS, CHANNELS), jnp.float32) * CHANNELS ** -0.5).astype(jnp.bfloat16)
    mix_bias = 0.5 * jax.random.normal(key_bias, (LAYERS, CHANNELS), jnp.float32)
    return {'volumes': volumes, 'filter_taps': filter_taps, 'mix_weight': mix_weight, 'mix_bias': mix_bias}


def line_filter(field_3d, tap_row, axis_dim):
    extent = field_3d.shape[axis_dim]
    pad_spec = [(0, 0), (0, 0), (0, 0)]
    pad_spec[axis_dim] = (HALF_WIDTH, HALF_WIDTH)
    padded = jnp.pad(field_3d.astype(jnp.float32), pad_spec)
    taps_used = tap_row.astype(jnp.bfloat16).astype(jnp.float32)
    acc_sum = jnp.zeros(field_3d.shape, jnp.float32)
    for offset in range(TAPS):
        acc_sum = acc_sum + taps_used[offset] * lax.slice_in_dim(padded, offset, offset + extent, axis=axis_dim)
    return acc_sum.astype(jnp.bfloat16)


def layer_step(vol_state, layer_params):
    tap_block, weight, bias_row = layer_params

    def one_volume(volume):
        def one_channel(field_3d):
            field_3d = line_filter(field_3d, tap_block[0], 0)
            field_3d = line_filter(field_3d, tap_block[1], 1)
            return line_filter(field_3d, tap_block[2], 2)

        filtered = lax.map(one_channel, volume)
        flat_units = filtered.reshape(CHANNELS, -1)
        mix_out = jnp.dot(weight.T, flat_units, preferred_element_type=jnp.float32).reshape(volume.shape)
        activated = jax.nn.gelu(mix_out + bias_row[:, None, None, None], approximate=True)
        return (volume.astype(jnp.float32) + activated).astype(jnp.bfloat16)

    return lax.map(one_volume, vol_state), None


def reference(volumes, filter_taps, mix_weight, mix_bias):
    outcome = lax.scan(layer_step, volumes, (filter_taps, mix_weight, mix_bias))
    return outcome[0]
```

```python
import functools

import jax
import jax.numpy as jnp
from jax import lax
from jax.experimental import pallas as pl
from jax.experimental.pallas import tpu as pltpu
from jax.sharding import PartitionSpec as P


BF = jnp.bfloat16
F32 = jnp.float32
SUB = 4
ROWS = SUB * SUB
PITCH = 40


def shape_of(*dims, dtype=BF):
    return jax.ShapeDtypeStruct(dims, dtype)


def grid2(rows, cols):
    return lax.broadcasted_iota(jnp.int32, (rows, cols), 0), lax.broadcasted_iota(jnp.int32, (rows, cols), 1)


def interleave(first, second):
    return jnp.concatenate([first, second], axis=1)


def bands_kernel(taps_ref, iband_ref, jband_ref, kband_ref, khalo_ref):
    layer = pl.program_id(0)
    at_end = lax.axis_index('pz') == 0
    half = (taps_ref.shape[2] - 1) // 2

    def toeplitz(ref, axis, out_pos, in_pos, keep):
        tap = jnp.where(keep, in_pos - out_pos + half, -1)
        total = jnp.zeros(tap.shape, F32)
        for t in range(2 * half + 1):
            total = jnp.where(tap == t, taps_ref[layer, axis, t], total)
        ref[0] = total.astype(BF)

    def rows_cols(ref):
        dims = ref.shape[1:]
        return lax.broadcasted_iota(jnp.int32, dims, 0), lax.broadcasted_iota(jnp.int32, dims, 1)

    lanes = iband_ref.shape[1] // 2
    o, n = rows_cols(iband_ref)
    toeplitz(iband_ref, 0, n % lanes, o % lanes, o // lanes == n // lanes)
    o, n = rows_cols(jband_ref)
    toeplitz(jband_ref, 1, o // SUB, n // SUB - half, o % SUB == n % SUB)
    groups = kband_ref.shape[1] // ROWS
    edge = khalo_ref.shape[1] // ROWS

    def k_of(row):
        turned = row // ROWS + jnp.where(at_end, groups - edge, 0)
        return jnp.where(turned >= groups, turned - groups, turned) * SUB + row % SUB

    def same_j(o, n):
        return (o % ROWS) // SUB == (n % ROWS) // SUB

    o, n = rows_cols(kband_ref)
    toeplitz(kband_ref, 2, k_of(o), k_of(n), same_j(o, n))
    o, n = rows_cols(khalo_ref)
    far = jnp.where(at_end, groups * SUB, -half) + (n // ROWS) * SUB + n % SUB
    toeplitz(khalo_ref, 2, k_of(o), far, same_j(o, n))


def bands(taps, lanes, j_len, kg, hg):
    layers, _, count = taps.shape
    sizes = [(2 * lanes, 2 * lanes), (j_len * SUB, (j_len + count - 1) * SUB), (kg * ROWS,) * 2, (hg * ROWS,) * 2]
    return pl.pallas_call(
        bands_kernel,
        out_shape=[shape_of(layers, *s) for s in sizes],
        grid=(layers,),
        in_specs=[pl.BlockSpec(memory_space=pltpu.SMEM)],
        out_specs=[pl.BlockSpec((1,) + s, lambda l: (l, 0, 0)) for s in sizes],
        compiler_params=pltpu.CompilerParams(dimension_semantics=("arbitrary",)),
        name='bands',
    )(taps)


def enter_kernel(half_ref, own_ref, other_ref, perm_ref, band_ref, *refs):
    vol_ref, filt_ref, upn_ref, upd_ref, dnn_ref, dnd_ref, scratch = refs[-7:]
    side, j_len, k_len = own_ref.shape[2], own_ref.shape[3], own_ref.shape[4]
    lanes = 2 * side
    first = half_ref[0] * side

    def fill(n, _):
        for base, ref in ((first, own_ref), (side - first, other_ref)):
            pair = interleave(ref[0, 0, n], ref[0, 1, n]).astype(F32)
            scratch[pl.ds(pl.multiple_of((base + n) * PITCH, 8), j_len), :] = pair
        return 0

    lax.fori_loop(0, side, fill, 0, unroll=8)

    def group(g, _):
        tiles = [scratch[pl.ds(g * SUB + j, lanes, stride=PITCH), :].T.astype(BF) for j in range(SUB)]
        columns = interleave(
            jnp.concatenate([t[:k_len] for t in tiles], axis=0),
            jnp.concatenate([t[k_len:] for t in tiles], axis=0),
        )
        mixed = jnp.dot(perm_ref[...], columns, preferred_element_type=F32).astype(BF)
        filtered = jnp.dot(mixed, band_ref[...], preferred_element_type=F32).astype(BF)
        for m in range(2):
            vol_ref[g, :, m] = mixed[:, m * lanes:(m + 1) * lanes].reshape(-1, ROWS, lanes)
            filt_ref[g, :, m] = filtered[:, m * lanes:(m + 1) * lanes].reshape(-1, ROWS, lanes)
        return 0

    groups = j_len // SUB
    lax.fori_loop(0, groups, group, 0, unroll=4)
    hg = upn_ref.shape[0]
    upn_ref[...] = filt_ref[groups - hg:, :hg]
    upd_ref[...] = filt_ref[groups - hg:, hg:]
    dnn_ref[...] = filt_ref[:hg, :hg]
    dnd_ref[...] = filt_ref[:hg, hg:]


def enter(volumes, vol_idx, other, chan_at, before, half, perm, band, hg):
    _, chans, side, j_all, k_len = volumes.shape
    j_len = j_all // 2
    jg, kg = j_len // SUB, k_len // SUB
    at = chan_at // 2
    sizes = [(jg, kg), (jg, kg), (hg, hg), (hg, kg - hg), (hg, hg), (hg, kg - hg)]
    before = before or []
    return pl.pallas_call(
        enter_kernel,
        out_shape=[shape_of(*s, chans, ROWS, 2 * side) for s in sizes],
        grid_spec=pltpu.PrefetchScalarGridSpec(
            num_scalar_prefetch=1,
            grid=(other.shape[1] // 2,),
            in_specs=[
                pl.BlockSpec((1, 2, side, j_len, k_len), lambda c, h: (vol_idx, c + at, 0, h[0], 0)),
                pl.BlockSpec((1, 2, side, j_len, k_len), lambda c, h: (0, c, 0, 0, 0)),
                pl.BlockSpec(perm.shape, lambda c, h: (0, 0)),
                pl.BlockSpec((None,) + band.shape[1:], lambda c, h: (0, 0, 0)),
            ] + [pl.BlockSpec(memory_space=pl.ANY)] * len(before),
            out_specs=[pl.BlockSpec(s + (2, ROWS, 2 * side), lambda c, h: (0, 0, c + at, 0, 0)) for s in sizes],
            scratch_shapes=[pltpu.VMEM((2 * side * PITCH, 2 * k_len), F32)],
        ),
        input_output_aliases={5 + n: n for n in range(len(before))},
        compiler_params=pltpu.CompilerParams(dimension_semantics=("arbitrary",)),
        cost_estimate=pl.CostEstimate(flops=other.shape[1] * 1_000_000_000, bytes_accessed=other.shape[1] * 2_500_000, transcendentals=0),
    )(half, volumes, other, perm, band, *before)


def leave_kernel(half_ref, own_ref, other_ref, perm_ref, *refs):
    raw_ref, scratch = refs[-2:]
    side, j_all, k_len = raw_ref.shape[2], raw_ref.shape[3], raw_ref.shape[4]
    lanes = own_ref.shape[4]
    j_len = j_all // 2
    half = half_ref[0]
    left = lax.broadcasted_iota(jnp.int32, (own_ref.shape[1] * ROWS, lanes), 1) < side

    def group(g, _):
        chan = []
        for m in range(2):
            a, b = own_ref[g, :, m].reshape(-1, lanes), other_ref[g, :, m].reshape(-1, lanes)
            chan.append(jnp.concatenate([
                interleave(a[:, :side], b[:, :side]), interleave(a[:, side:], b[:, side:])], axis=0))
        rows = jnp.dot(perm_ref[...], interleave(*chan), preferred_element_type=F32)
        for j in range(SUB):
            part = rows[j * k_len:(j + 1) * k_len]
            tile = jnp.concatenate([part[:, :lanes], part[:, lanes:]], axis=0)
            scratch[pl.ds(g * SUB + j, lanes, stride=PITCH), :] = tile.T
        return 0

    lax.fori_loop(0, j_len // SUB, group, 0, unroll=4)

    def drain(n, _):
        for base, where in ((0, half), (side, 1 - half)):
            pair = scratch[pl.ds(pl.multiple_of((base + n) * PITCH, 8), j_len), :].astype(BF)
            at = pl.ds(pl.multiple_of(where * j_len, j_len), j_len)
            raw_ref[0, 0, n, at] = pair[:, :k_len]
            raw_ref[0, 1, n, at] = pair[:, k_len:]
        return 0

    lax.fori_loop(0, side, drain, 0, unroll=8)


def leave(own, other, vol_idx, result, half, perm, full_shape):
    _, chans, side, j_all, k_len = full_shape
    jg, kp = own.shape[:2]
    operands = [half, own, other, perm]
    spec = pl.BlockSpec((jg, kp, 2, ROWS, 2 * side), lambda c, h: (0, 0, c, 0, 0))
    in_specs = [spec, spec, pl.BlockSpec(perm.shape, lambda c, h: (0, 0))]
    aliases = {}
    if result is not None:
        operands.append(result)
        in_specs.append(pl.BlockSpec(memory_space=pl.ANY))
        aliases = {4: 0}
    return pl.pallas_call(
        leave_kernel,
        out_shape=shape_of(*full_shape),
        grid_spec=pltpu.PrefetchScalarGridSpec(
            num_scalar_prefetch=1,
            grid=(chans // 2,),
            in_specs=in_specs,
            out_specs=pl.BlockSpec((1, 2, side, j_all, k_len), lambda c, h: (vol_idx, c, 0, 0, 0)),
            scratch_shapes=[pltpu.VMEM((2 * side * PITCH, 2 * k_len), F32)],
        ),
        input_output_aliases=aliases,
        compiler_params=pltpu.CompilerParams(dimension_semantics=("arbitrary",)),
        cost_estimate=pl.CostEstimate(flops=30_000_000_000, bytes_accessed=50_000_000, transcendentals=0),
    )(*operands)


def along_j_kernel(field_ref, low_ref, high_ref, band_ref, out_ref):
    chans, lanes = field_ref.shape[2], field_ref.shape[4]

    def pair(n, _):
        halves = []
        for m in range(2):
            c = 2 * n + m
            halves.append(jnp.concatenate(
                [ref[:, 0, c].reshape(-1, lanes) for ref in (low_ref, field_ref, high_ref)], axis=0))
        total = jnp.dot(band_ref[...], interleave(*halves), preferred_element_type=F32).astype(BF)
        for m in range(2):
            out_ref[:, 0, 2 * n + m] = total[:, m * lanes:(m + 1) * lanes].reshape(-1, ROWS, lanes)
        return 0

    lax.fori_loop(0, chans // 2, pair, 0, unroll=4)


def along_j(field, low, high, band, layer, first):
    jg, _, chans, rows, lanes = field.shape
    halo, count = low.shape[:2]
    return pl.pallas_call(
        along_j_kernel,
        out_shape=shape_of(jg, count, chans, rows, lanes),
        grid=(count,),
        in_specs=[
            pl.BlockSpec((jg, 1, chans, rows, lanes), lambda g: (0, g + first, 0, 0, 0)),
            pl.BlockSpec((halo, 1, chans, rows, lanes), lambda g: (0, g, 0, 0, 0)),
            pl.BlockSpec((halo, 1, chans, rows, lanes), lambda g: (0, g, 0, 0, 0)),
            pl.BlockSpec((None,) + band.shape[1:], lambda g: (layer, 0, 0)),
        ],
        out_specs=pl.BlockSpec((jg, 1, chans, rows, lanes), lambda g: (0, g, 0, 0, 0)),
        compiler_params=pltpu.CompilerParams(dimension_semantics=("arbitrary",)),
        cost_estimate=pl.CostEstimate(flops=count * 1_000_000_000, bytes_accessed=count * 2_900_000, transcendentals=0),
    )(field, low, high, band)


GELU_A = 0.7978845608028654
GELU_B = GELU_A * 0.044715


def finish_kernel(last, edge_ref, rest_ref, halo_ref, vol_ref, band_ref, halo_band_ref, mix_ref, bias_ref, *refs):
    unit = refs[-1]
    edge = edge_ref.shape[1]
    groups, chans, lanes = vol_ref.shape[1], vol_ref.shape[2], vol_ref.shape[4]
    edge_rows = edge * ROWS

    def channel_pair(n, _):
        own, far = [], []
        for m in range(2):
            c = 2 * n + m
            own.append(jnp.concatenate(
                [edge_ref[0, :, c].reshape(-1, lanes), rest_ref[0, :, c].reshape(-1, lanes)], axis=0))
            far.append(halo_ref[0, :, c].reshape(-1, lanes))
        total = jnp.dot(band_ref[...], interleave(*own), preferred_element_type=F32)
        extra = jnp.dot(halo_band_ref[...], interleave(*far), preferred_element_type=F32)
        head = (total[:edge_rows] + extra).astype(BF)
        tail = total[edge_rows:].astype(BF)
        for m in range(2):
            cut = slice(m * lanes, (m + 1) * lanes)
            unit[:edge, 2 * n + m] = head[:, cut].reshape(-1, ROWS, lanes)
            unit[edge:, 2 * n + m] = tail[:, cut].reshape(-1, ROWS, lanes)
        return 0

    lax.fori_loop(0, chans // 2, channel_pair, 0, unroll=4)

    def group_pair(n, _):
        k0, k1 = (n, n + groups // 2) if last else (2 * n, 2 * n + 1)
        both = lambda ref, lead: interleave(
            ref[lead + (k0,)].reshape(-1, lanes), ref[lead + (k1,)].reshape(-1, lanes))
        x = jnp.dot(mix_ref[...], both(unit, ()), preferred_element_type=F32) + interleave(bias_ref[...], bias_ref[...])
        half_x = 0.5 * x
        act = half_x * jnp.tanh(x * (GELU_A + GELU_B * (x * x))) + half_x
        new = (both(vol_ref, (0,)).astype(F32) + act).astype(BF)
        shaped = lambda a: a.reshape(chans, ROWS, lanes)
        if last:
            own_ref, other_ref = refs[:2]
            side = lanes // 2
            low = interleave(new[:, :side], new[:, lanes:lanes + side])
            high = interleave(new[:, side:lanes], new[:, lanes + side:])
            is_low = lax.axis_index('px') == 0
            own_ref[0, n] = shaped(jnp.where(is_low, low, high))
            other_ref[0, n] = shaped(jnp.where(is_low, high, low))
        else:
            iband_ref, new_ref, filt_ref = refs[:3]
            new_ref[0, k0], new_ref[0, k1] = shaped(new[:, :lanes]), shaped(new[:, lanes:])
            filt = jnp.dot(new, iband_ref[...], preferred_element_type=F32).astype(BF)
            filt_ref[0, k0], filt_ref[0, k1] = shaped(filt[:, :lanes]), shaped(filt[:, lanes:])
        return 0

    lax.fori_loop(0, groups // 2, group_pair, 0, unroll=4)

    if not last:
        filt_ref, upn_ref, upd_ref, dnn_ref, dnd_ref = refs[2:7]
        g = pl.program_id(0)

        @pl.when(g < edge)
        def _():
            dnn_ref[0] = filt_ref[0, :edge]
            dnd_ref[0] = filt_ref[0, edge:]

        @pl.when(g >= pl.num_programs(0) - edge)
        def _():
            upn_ref[0] = filt_ref[0, :edge]
            upd_ref[0] = filt_ref[0, edge:]


def finish(edge, rest, halo, vol, layer, band, halo_band, mix, bias, iband):
    jg, kg, chans, rows, lanes = vol.shape
    hg = edge.shape[1]
    last = iband is None
    block = lambda a: pl.BlockSpec((1,) + a.shape[1:], lambda g: (g, 0, 0, 0, 0))
    of_layer = lambda a, l: pl.BlockSpec((None,) + a.shape[1:], lambda g: (l, 0, 0))
    in_specs = [block(edge), block(rest), block(halo), block(vol)]
    in_specs += [of_layer(a, layer) for a in (band, halo_band, mix, bias)]
    operands = [edge, rest, halo, vol, band, halo_band, mix, bias]
    if last:
        packed = shape_of(jg, kg // 2, chans, rows, lanes)
        out_shape, out_specs = [packed] * 2, [block(packed)] * 2
    else:
        operands.append(iband)
        in_specs.append(of_layer(iband, layer + 1))
        out_shape = [shape_of(*vol.shape)] * 2
        out_specs = [block(vol)] * 2
        up = lambda g: (jnp.maximum(g - (jg - hg), 0), 0, 0, 0, 0)
        down = lambda g: (jnp.minimum(g, hg - 1), 0, 0, 0, 0)
        for index in (up, down):
            for size in (hg, kg - hg):
                out_shape.append(shape_of(hg, size, chans, rows, lanes))
                out_specs.append(pl.BlockSpec((1, size, chans, rows, lanes), index))
    return pl.pallas_call(
        functools.partial(finish_kernel, last),
        out_shape=out_shape,
        grid=(jg,),
        in_specs=in_specs,
        out_specs=out_specs,
        scratch_shapes=[pltpu.VMEM((kg, chans, rows, lanes), BF)],
        compiler_params=pltpu.CompilerParams(dimension_semantics=("arbitrary",)),
        cost_estimate=pl.CostEstimate(flops=40_000_000_000, bytes_accessed=75_000_000, transcendentals=8_400_000),
    )(*operands)


def solution(mesh):
    sizes = {a: mesh.shape[a] for a in ('px', 'py', 'pz')}
    vol_spec = P('dp', None, 'px', 'py', 'pz')

    def local_layers(volumes, filter_taps, mix_weight, mix_bias):
        count, chans, side, j_all, k_len = volumes.shape
        layers, _, taps = filter_taps.shape
        half = (taps - 1) // 2
        j_len = j_all // 2
        kg, hg = k_len // SUB, half // SUB
        px, pz = lax.axis_index('px'), lax.axis_index('pz')
        half_idx = px.astype(jnp.int32).reshape(1)
        iband, jband, kband, khalo = bands(filter_taps.astype(BF).astype(F32), 2 * side, j_len, kg, hg)

        o, n = grid2(chans * ROWS, chans * ROWS)
        spread = jnp.repeat(jnp.repeat(mix_weight.swapaxes(1, 2), ROWS, axis=1), ROWS, axis=2)
        mix = jnp.where(o % ROWS == n % ROWS, spread, jnp.zeros((), BF))
        bias = jnp.broadcast_to(jnp.repeat(mix_bias, ROWS, axis=1)[:, :, None], (layers, chans * ROWS, 2 * side))

        o, n = grid2(kg * ROWS, SUB * k_len)
        k_row = jnp.where(pz == 0, (o // ROWS + kg - hg) % kg, o // ROWS) * SUB + o % SUB
        perm = jnp.where(n == ((o % ROWS) // SUB) * k_len + k_row, 1.0, 0.0).astype(BF)

        swap = [(0, 1), (1, 0)]
        line = sizes['py'] * sizes['px']
        upward = [(s, s + 1) for s in range(line - 1)]
        downward = [(s + 1, s) for s in range(line - 1)]
        up = lambda a: lax.ppermute(a, ('py', 'px'), upward)
        down = lambda a: lax.ppermute(a, ('py', 'px'), downward)

        states = []
        for v in range(count):
            pieces = 2 if v == 0 else 1
            width = chans // pieces
            outs = None
            for p in range(pieces):
                sent = lax.dynamic_slice(
                    volumes, (v, p * width, 0, (1 - px) * j_len, 0), (1, width, side, j_len, k_len))
                other = lax.ppermute(sent, 'px', swap)
                outs = enter(volumes, v, other, p * width, outs, half_idx, perm, iband, hg)
            states.append(outs)
        result = None

        def send_j(v):
            _, _, up_near, up_deep, down_near, down_deep = states[v]
            moved = []
            for move, part in ((up, up_near), (down, down_near),
                                     (up, up_deep), (down, down_deep)):
                moved.append(move(part))
            return moved

        def edge_of(l, v, after):
            filt = states[v][1]
            if after is not None:
                filt, after = lax.optimization_barrier((filt, after))
            edge = along_j(filt, *halos[v][:2], jband, l, 0)
            return edge, lax.ppermute(edge, 'pz', swap), after

        halos = [send_j(v) for v in range(count)]
        edges = [edge_of(0, 0, None)] + [None] * (count - 1)
        rests = [None] * count
        rests[0] = along_j(states[0][1], *halos[0][2:], jband, 0, hg)
        for step in range(count * layers):
            l, v = divmod(step, count)
            nl, nv = divmod(step + 1, count)
            if nl < layers and edges[nv] is None:
                edges[nv] = edge_of(nl, nv, rests[v])
                rests[v] = edges[nv][2]
            edge, halo, _ = edges[v]
            states[v] = finish(edge, rests[v], halo, states[v][0], l, kband, khalo, mix, bias,
                               iband if l + 1 < layers else None)
            edges[v] = rests[v] = None
            if l + 1 < layers:
                halos[v] = send_j(v)
            if nl < layers:
                rests[nv] = along_j(states[nv][1], *halos[nv][2:], jband, nl, hg)
        for v in range(count):
            own, other = states[v]
            other = lax.ppermute(other, 'px', swap)
            result = leave(own, other, v, result, half_idx, perm.T, volumes.shape)
        return result

    return jax.shard_map(local_layers, mesh=mesh, in_specs=(vol_spec, P(), P(), P()), out_specs=vol_spec, check_vma=False)
```

```python
import functools

import jax
import jax.numpy as jnp
from jax import lax
from jax.experimental import pallas as pl
from jax.experimental.pallas import tpu as pltpu
from jax.sharding import PartitionSpec as P


BF = jnp.bfloat16
F32 = jnp.float32
SUB = 4
ROWS = SUB * SUB
PITCH = 40


def shape_of(*dims, dtype=BF):
    return jax.ShapeDtypeStruct(dims, dtype)


def grid2(rows, cols):
    return lax.broadcasted_iota(jnp.int32, (rows, cols), 0), lax.broadcasted_iota(jnp.int32, (rows, cols), 1)


def interleave(first, second):
    return jnp.concatenate([first, second], axis=1)


def bands_kernel(taps_ref, iband_ref, jband_ref, kband_ref, khalo_ref):
    layer = pl.program_id(0)
    at_end = lax.axis_index('pz') == 0
    half = (taps_ref.shape[2] - 1) // 2

    def toeplitz(ref, axis, out_pos, in_pos, keep):
        tap = jnp.where(keep, in_pos - out_pos + half, -1)
        total = jnp.zeros(tap.shape, F32)
        for t in range(2 * half + 1):
            total = jnp.where(tap == t, taps_ref[layer, axis, t], total)
        ref[0] = total.astype(BF)

    def rows_cols(ref):
        dims = ref.shape[1:]
        return lax.broadcasted_iota(jnp.int32, dims, 0), lax.broadcasted_iota(jnp.int32, dims, 1)

    lanes = iband_ref.shape[1] // 2
    o, n = rows_cols(iband_ref)
    toeplitz(iband_ref, 0, n % lanes, o % lanes, o // lanes == n // lanes)
    o, n = rows_cols(jband_ref)
    toeplitz(jband_ref, 1, o // SUB, n // SUB - half, o % SUB == n % SUB)
    groups = kband_ref.shape[1] // ROWS
    edge = khalo_ref.shape[1] // ROWS

    def k_of(row):
        turned = row // ROWS + jnp.where(at_end, groups - edge, 0)
        return jnp.where(turned >= groups, turned - groups, turned) * SUB + row % SUB

    def same_j(o, n):
        return (o % ROWS) // SUB == (n % ROWS) // SUB

    o, n = rows_cols(kband_ref)
    toeplitz(kband_ref, 2, k_of(o), k_of(n), same_j(o, n))
    o, n = rows_cols(khalo_ref)
    far = jnp.where(at_end, groups * SUB, -half) + (n // ROWS) * SUB + n % SUB
    toeplitz(khalo_ref, 2, k_of(o), far, same_j(o, n))


def bands(taps, lanes, j_len, kg, hg):
    layers, _, count = taps.shape
    sizes = [(2 * lanes, 2 * lanes), (j_len * SUB, (j_len + count - 1) * SUB), (kg * ROWS,) * 2, (hg * ROWS,) * 2]
    return pl.pallas_call(
        bands_kernel,
        out_shape=[shape_of(layers, *s) for s in sizes],
        grid=(layers,),
        in_specs=[pl.BlockSpec(memory_space=pltpu.SMEM)],
        out_specs=[pl.BlockSpec((1,) + s, lambda l: (l, 0, 0)) for s in sizes],
        compiler_params=pltpu.CompilerParams(dimension_semantics=("arbitrary",)),
        name='bands',
    )(taps)


def enter_kernel(half_ref, own_ref, other_ref, perm_ref, band_ref, *refs):
    vol_ref, filt_ref, upn_ref, upd_ref, dnn_ref, dnd_ref, scratch = refs[-7:]
    side, j_len, k_len = own_ref.shape[2], own_ref.shape[3], own_ref.shape[4]
    lanes = 2 * side
    first = half_ref[0] * side

    def fill(n, _):
        for base, ref in ((first, own_ref), (side - first, other_ref)):
            pair = interleave(ref[0, 0, n], ref[0, 1, n]).astype(F32)
            scratch[pl.ds(pl.multiple_of((base + n) * PITCH, 8), j_len), :] = pair
        return 0

    lax.fori_loop(0, side, fill, 0, unroll=16)

    def group(g, _):
        tiles = [scratch[pl.ds(g * SUB + j, lanes, stride=PITCH), :].T.astype(BF) for j in range(SUB)]
        columns = interleave(
            jnp.concatenate([t[:k_len] for t in tiles], axis=0),
            jnp.concatenate([t[k_len:] for t in tiles], axis=0),
        )
        mixed = jnp.dot(perm_ref[...], columns, preferred_element_type=F32).astype(BF)
        filtered = jnp.dot(mixed, band_ref[...], preferred_element_type=F32).astype(BF)
        for m in range(2):
            vol_ref[g, :, m] = mixed[:, m * lanes:(m + 1) * lanes].reshape(-1, ROWS, lanes)
            filt_ref[g, :, m] = filtered[:, m * lanes:(m + 1) * lanes].reshape(-1, ROWS, lanes)
        return 0

    groups = j_len // SUB
    lax.fori_loop(0, groups, group, 0, unroll=8)
    hg = upn_ref.shape[0]
    upn_ref[...] = filt_ref[groups - hg:, :hg]
    upd_ref[...] = filt_ref[groups - hg:, hg:]
    dnn_ref[...] = filt_ref[:hg, :hg]
    dnd_ref[...] = filt_ref[:hg, hg:]


def enter(volumes, vol_idx, other, chan_at, before, half, perm, band, hg):
    _, chans, side, j_all, k_len = volumes.shape
    j_len = j_all // 2
    jg, kg = j_len // SUB, k_len // SUB
    at = chan_at // 2
    sizes = [(jg, kg), (jg, kg), (hg, hg), (hg, kg - hg), (hg, hg), (hg, kg - hg)]
    before = before or []
    return pl.pallas_call(
        enter_kernel,
        out_shape=[shape_of(*s, chans, ROWS, 2 * side) for s in sizes],
        grid_spec=pltpu.PrefetchScalarGridSpec(
            num_scalar_prefetch=1,
            grid=(other.shape[1] // 2,),
            in_specs=[
                pl.BlockSpec((1, 2, side, j_len, k_len), lambda c, h: (vol_idx, c + at, 0, h[0], 0)),
                pl.BlockSpec((1, 2, side, j_len, k_len), lambda c, h: (0, c, 0, 0, 0)),
                pl.BlockSpec(perm.shape, lambda c, h: (0, 0)),
                pl.BlockSpec((None,) + band.shape[1:], lambda c, h: (0, 0, 0)),
            ] + [pl.BlockSpec(memory_space=pl.ANY)] * len(before),
            out_specs=[pl.BlockSpec(s + (2, ROWS, 2 * side), lambda c, h: (0, 0, c + at, 0, 0)) for s in sizes],
            scratch_shapes=[pltpu.VMEM((2 * side * PITCH, 2 * k_len), F32)],
        ),
        input_output_aliases={5 + n: n for n in range(len(before))},
        compiler_params=pltpu.CompilerParams(dimension_semantics=("arbitrary",)),
        cost_estimate=pl.CostEstimate(flops=other.shape[1] * 1_000_000_000, bytes_accessed=other.shape[1] * 2_500_000, transcendentals=0),
    )(half, volumes, other, perm, band, *before)


def leave_kernel(half_ref, own_ref, other_ref, perm_ref, *refs):
    raw_ref, scratch = refs[-2:]
    side, j_all, k_len = raw_ref.shape[2], raw_ref.shape[3], raw_ref.shape[4]
    lanes = own_ref.shape[4]
    j_len = j_all // 2
    half = half_ref[0]
    left = lax.broadcasted_iota(jnp.int32, (own_ref.shape[1] * ROWS, lanes), 1) < side

    def group(g, _):
        chan = []
        for m in range(2):
            a, b = own_ref[g, :, m].reshape(-1, lanes), other_ref[g, :, m].reshape(-1, lanes)
            chan.append(jnp.concatenate([
                interleave(a[:, :side], b[:, :side]), interleave(a[:, side:], b[:, side:])], axis=0))
        rows = jnp.dot(perm_ref[...], interleave(*chan), preferred_element_type=F32)
        for j in range(SUB):
            part = rows[j * k_len:(j + 1) * k_len]
            tile = jnp.concatenate([part[:, :lanes], part[:, lanes:]], axis=0)
            scratch[pl.ds(g * SUB + j, lanes, stride=PITCH), :] = tile.T
        return 0

    lax.fori_loop(0, j_len // SUB, group, 0, unroll=8)

    def drain(n, _):
        for base, where in ((0, half), (side, 1 - half)):
            pair = scratch[pl.ds(pl.multiple_of((base + n) * PITCH, 8), j_len), :].astype(BF)
            at = pl.ds(pl.multiple_of(where * j_len, j_len), j_len)
            raw_ref[0, 0, n, at] = pair[:, :k_len]
            raw_ref[0, 1, n, at] = pair[:, k_len:]
        return 0

    lax.fori_loop(0, side, drain, 0, unroll=16)


def leave(own, other, vol_idx, result, half, perm, full_shape):
    _, chans, side, j_all, k_len = full_shape
    jg, kp = own.shape[:2]
    operands = [half, own, other, perm]
    spec = pl.BlockSpec((jg, kp, 2, ROWS, 2 * side), lambda c, h: (0, 0, c, 0, 0))
    in_specs = [spec, spec, pl.BlockSpec(perm.shape, lambda c, h: (0, 0))]
    aliases = {}
    if result is not None:
        operands.append(result)
        in_specs.append(pl.BlockSpec(memory_space=pl.ANY))
        aliases = {4: 0}
    return pl.pallas_call(
        leave_kernel,
        out_shape=shape_of(*full_shape),
        grid_spec=pltpu.PrefetchScalarGridSpec(
            num_scalar_prefetch=1,
            grid=(chans // 2,),
            in_specs=in_specs,
            out_specs=pl.BlockSpec((1, 2, side, j_all, k_len), lambda c, h: (vol_idx, c, 0, 0, 0)),
            scratch_shapes=[pltpu.VMEM((2 * side * PITCH, 2 * k_len), F32)],
        ),
        input_output_aliases=aliases,
        compiler_params=pltpu.CompilerParams(dimension_semantics=("arbitrary",)),
        cost_estimate=pl.CostEstimate(flops=30_000_000_000, bytes_accessed=50_000_000, transcendentals=0),
    )(*operands)


def along_j_kernel(field_ref, low_ref, high_ref, band_ref, out_ref):
    chans, lanes = field_ref.shape[2], field_ref.shape[4]

    def pair(n, _):
        halves = []
        for m in range(2):
            c = 2 * n + m
            halves.append(jnp.concatenate(
                [ref[:, 0, c].reshape(-1, lanes) for ref in (low_ref, field_ref, high_ref)], axis=0))
        total = jnp.dot(band_ref[...], interleave(*halves), preferred_element_type=F32).astype(BF)
        for m in range(2):
            out_ref[:, 0, 2 * n + m] = total[:, m * lanes:(m + 1) * lanes].reshape(-1, ROWS, lanes)
        return 0

    lax.fori_loop(0, chans // 2, pair, 0, unroll=4)


def along_j(field, low, high, band, layer, first):
    jg, _, chans, rows, lanes = field.shape
    halo, count = low.shape[:2]
    return pl.pallas_call(
        along_j_kernel,
        out_shape=shape_of(jg, count, chans, rows, lanes),
        grid=(count,),
        in_specs=[
            pl.BlockSpec((jg, 1, chans, rows, lanes), lambda g: (0, g + first, 0, 0, 0)),
            pl.BlockSpec((halo, 1, chans, rows, lanes), lambda g: (0, g, 0, 0, 0)),
            pl.BlockSpec((halo, 1, chans, rows, lanes), lambda g: (0, g, 0, 0, 0)),
            pl.BlockSpec((None,) + band.shape[1:], lambda g: (layer, 0, 0)),
        ],
        out_specs=pl.BlockSpec((jg, 1, chans, rows, lanes), lambda g: (0, g, 0, 0, 0)),
        compiler_params=pltpu.CompilerParams(dimension_semantics=("arbitrary",)),
        cost_estimate=pl.CostEstimate(flops=count * 1_000_000_000, bytes_accessed=count * 2_900_000, transcendentals=0),
    )(field, low, high, band)


GELU_A = 0.7978845608028654
GELU_B = GELU_A * 0.044715


def finish_kernel(last, edge_ref, rest_ref, halo_ref, vol_ref, band_ref, halo_band_ref, mix_ref, bias_ref, *refs):
    unit = refs[-1]
    edge = edge_ref.shape[1]
    groups, chans, lanes = vol_ref.shape[1], vol_ref.shape[2], vol_ref.shape[4]
    edge_rows = edge * ROWS

    def channel_pair(n, _):
        own, far = [], []
        for m in range(2):
            c = 2 * n + m
            own.append(jnp.concatenate(
                [edge_ref[0, :, c].reshape(-1, lanes), rest_ref[0, :, c].reshape(-1, lanes)], axis=0))
            far.append(halo_ref[0, :, c].reshape(-1, lanes))
        total = jnp.dot(band_ref[...], interleave(*own), preferred_element_type=F32)
        extra = jnp.dot(halo_band_ref[...], interleave(*far), preferred_element_type=F32)
        head = (total[:edge_rows] + extra).astype(BF)
        tail = total[edge_rows:].astype(BF)
        for m in range(2):
            cut = slice(m * lanes, (m + 1) * lanes)
            unit[:edge, 2 * n + m] = head[:, cut].reshape(-1, ROWS, lanes)
            unit[edge:, 2 * n + m] = tail[:, cut].reshape(-1, ROWS, lanes)
        return 0

    lax.fori_loop(0, chans // 2, channel_pair, 0, unroll=chans // 2)

    def group_pair(n, _):
        k0, k1 = (n, n + groups // 2) if last else (2 * n, 2 * n + 1)
        both = lambda ref, lead: interleave(
            ref[lead + (k0,)].reshape(-1, lanes), ref[lead + (k1,)].reshape(-1, lanes))
        x = jnp.dot(mix_ref[...], both(unit, ()), preferred_element_type=F32) + interleave(bias_ref[...], bias_ref[...])
        half_x = 0.5 * x
        act = half_x * jnp.tanh(x * (GELU_A + GELU_B * (x * x))) + half_x
        new = (both(vol_ref, (0,)).astype(F32) + act).astype(BF)
        shaped = lambda a: a.reshape(chans, ROWS, lanes)
        if last:
            own_ref, other_ref = refs[:2]
            side = lanes // 2
            low = interleave(new[:, :side], new[:, lanes:lanes + side])
            high = interleave(new[:, side:lanes], new[:, lanes + side:])
            is_low = lax.axis_index('px') == 0
            own_ref[0, n] = shaped(jnp.where(is_low, low, high))
            other_ref[0, n] = shaped(jnp.where(is_low, high, low))
        else:
            new_ref = refs[1]
            new_ref[0, k0], new_ref[0, k1] = shaped(new[:, :lanes]), shaped(new[:, lanes:])
        return 0

    lax.fori_loop(0, groups // 2, group_pair, 0, unroll=4)

    if not last:
        iband_ref, new_ref, filt_ref, upn_ref, upd_ref, dnn_ref, dnd_ref = refs[:7]
        g = pl.program_id(0)
        many = groups // 2

        def along_i(n, _):
            first = n * many
            pairs = [interleave(new_ref[0, first + q].reshape(-1, lanes), new_ref[0, first + many // 2 + q].reshape(-1, lanes))
                     for q in range(many // 2)]
            filt = jnp.dot(jnp.concatenate(pairs, axis=0), iband_ref[...], preferred_element_type=F32).astype(BF)
            side_by_side = (filt[:, :lanes], filt[:, lanes:])
            for m in range(2):
                at = pl.ds(first + m * (many // 2), many // 2)
                filt_ref[0, at] = side_by_side[m].reshape(many // 2, chans, ROWS, lanes)
            return 0

        lax.fori_loop(0, groups // many, along_i, 0, unroll=2)

        @pl.when(g < edge)
        def _():
            dnn_ref[0] = filt_ref[0, :edge]
            dnd_ref[0] = filt_ref[0, edge:]

        @pl.when(g >= pl.num_programs(0) - edge)
        def _():
            upn_ref[0] = filt_ref[0, :edge]
            upd_ref[0] = filt_ref[0, edge:]


def finish(edge, rest, halo, vol, layer, band, halo_band, mix, bias, iband):
    jg, kg, chans, rows, lanes = vol.shape
    hg = edge.shape[1]
    last = iband is None
    block = lambda a: pl.BlockSpec((1,) + a.shape[1:], lambda g: (g, 0, 0, 0, 0))
    of_layer = lambda a, l: pl.BlockSpec((None,) + a.shape[1:], lambda g: (l, 0, 0))
    in_specs = [block(edge), block(rest), block(halo), block(vol)]
    in_specs += [of_layer(a, layer) for a in (band, halo_band, mix, bias)]
    operands = [edge, rest, halo, vol, band, halo_band, mix, bias]
    if last:
        packed = shape_of(jg, kg // 2, chans, rows, lanes)
        out_shape, out_specs = [packed] * 2, [block(packed)] * 2
    else:
        operands.append(iband)
        in_specs.append(of_layer(iband, layer + 1))
        out_shape = [shape_of(*vol.shape)] * 2
        out_specs = [block(vol)] * 2
        up = lambda g: (jnp.maximum(g - (jg - hg), 0), 0, 0, 0, 0)
        down = lambda g: (jnp.minimum(g, hg - 1), 0, 0, 0, 0)
        for index in (up, down):
            for size in (hg, kg - hg):
                out_shape.append(shape_of(hg, size, chans, rows, lanes))
                out_specs.append(pl.BlockSpec((1, size, chans, rows, lanes), index))
    return pl.pallas_call(
        functools.partial(finish_kernel, last),
        out_shape=out_shape,
        grid=(jg,),
        in_specs=in_specs,
        out_specs=out_specs,
        scratch_shapes=[pltpu.VMEM((kg, chans, rows, lanes), BF)],
        compiler_params=pltpu.CompilerParams(dimension_semantics=("arbitrary",)),
        cost_estimate=pl.CostEstimate(flops=40_000_000_000, bytes_accessed=75_000_000, transcendentals=8_400_000),
    )(*operands)


def solution(mesh):
    sizes = {a: mesh.shape[a] for a in ('px', 'py', 'pz')}
    vol_spec = P('dp', None, 'px', 'py', 'pz')

    def local_layers(volumes, filter_taps, mix_weight, mix_bias):
        count, chans, side, j_all, k_len = volumes.shape
        layers, _, taps = filter_taps.shape
        half = (taps - 1) // 2
        j_len = j_all // 2
        kg, hg = k_len // SUB, half // SUB
        px, pz = lax.axis_index('px'), lax.axis_index('pz')
        half_idx = px.astype(jnp.int32).reshape(1)
        iband, jband, kband, khalo = bands(filter_taps.astype(BF).astype(F32), 2 * side, j_len, kg, hg)

        o, n = grid2(chans * ROWS, chans * ROWS)
        spread = jnp.repeat(jnp.repeat(mix_weight.swapaxes(1, 2), ROWS, axis=1), ROWS, axis=2)
        mix = jnp.where(o % ROWS == n % ROWS, spread, jnp.zeros((), BF))
        bias = jnp.broadcast_to(jnp.repeat(mix_bias, ROWS, axis=1)[:, :, None], (layers, chans * ROWS, 2 * side))

        o, n = grid2(kg * ROWS, SUB * k_len)
        k_row = jnp.where(pz == 0, (o // ROWS + kg - hg) % kg, o // ROWS) * SUB + o % SUB
        perm = jnp.where(n == ((o % ROWS) // SUB) * k_len + k_row, 1.0, 0.0).astype(BF)

        swap = [(0, 1), (1, 0)]
        line = sizes['py'] * sizes['px']
        upward = [(s, s + 1) for s in range(line - 1)]
        downward = [(s + 1, s) for s in range(line - 1)]
        up = lambda a: lax.ppermute(a, ('py', 'px'), upward)
        down = lambda a: lax.ppermute(a, ('py', 'px'), downward)

        states = []
        for v in range(count):
            pieces = 2 if v == 0 else 1
            width = chans // pieces
            outs = None
            for p in range(pieces):
                sent = lax.dynamic_slice(
                    volumes, (v, p * width, 0, (1 - px) * j_len, 0), (1, width, side, j_len, k_len))
                other = lax.ppermute(sent, 'px', swap)
                outs = enter(volumes, v, other, p * width, outs, half_idx, perm, iband, hg)
            states.append(outs)
        result = None

        def send_j(v):
            _, _, up_near, up_deep, down_near, down_deep = states[v]
            moved = []
            for move, part in ((up, up_near), (down, down_near),
                                     (up, up_deep), (down, down_deep)):
                moved.append(move(part))
            return moved

        def edge_of(l, v, after):
            filt = states[v][1]
            if after is not None:
                filt, after = lax.optimization_barrier((filt, after))
            edge = along_j(filt, *halos[v][:2], jband, l, 0)
            return edge, lax.ppermute(edge, 'pz', swap), after

        halos = [send_j(v) for v in range(count)]
        edges = [edge_of(0, 0, None)] + [None] * (count - 1)
        rests = [None] * count
        rests[0] = along_j(states[0][1], *halos[0][2:], jband, 0, hg)
        for step in range(count * layers):
            l, v = divmod(step, count)
            nl, nv = divmod(step + 1, count)
            if nl < layers and edges[nv] is None:
                edges[nv] = edge_of(nl, nv, rests[v])
                rests[v] = edges[nv][2]
            edge, halo, _ = edges[v]
            states[v] = finish(edge, rests[v], halo, states[v][0], l, kband, khalo, mix, bias,
                               iband if l + 1 < layers else None)
            edges[v] = rests[v] = None
            if l + 1 < layers:
                halos[v] = send_j(v)
            if nl < layers:
                rests[nv] = along_j(states[nv][1], *halos[nv][2:], jband, nl, hg)
        for v in range(count):
            own, other = states[v]
            other = lax.ppermute(other, 'px', swap)
            result = leave(own, other, v, result, half_idx, perm.T, volumes.shape)
        return result

    return jax.shard_map(local_layers, mesh=mesh, in_specs=(vol_spec, P(), P(), P()), out_specs=vol_spec, check_vma=False)
```

```python
import functools

import jax
import jax.numpy as jnp
from jax import lax
from jax.experimental import pallas as pl
from jax.experimental.pallas import tpu as pltpu
from jax.sharding import PartitionSpec as P


BF = jnp.bfloat16
F32 = jnp.float32
SUB = 4
ROWS = SUB * SUB
PITCH = 40
CHAN_STEP = 8


def shape_of(*dims, dtype=BF):
    return jax.ShapeDtypeStruct(dims, dtype)


def grid2(rows, cols):
    return lax.broadcasted_iota(jnp.int32, (rows, cols), 0), lax.broadcasted_iota(jnp.int32, (rows, cols), 1)


def interleave(first, second):
    return jnp.concatenate([first, second], axis=1)


def bands_kernel(taps_ref, iband_ref, jband_ref, kband_ref, khalo_ref):
    layer = pl.program_id(0)
    at_end = lax.axis_index('pz') == 0
    half = (taps_ref.shape[2] - 1) // 2

    def toeplitz(ref, axis, out_pos, in_pos, keep):
        tap = jnp.where(keep, in_pos - out_pos + half, -1)
        total = jnp.zeros(tap.shape, F32)
        for t in range(2 * half + 1):
            total = jnp.where(tap == t, taps_ref[layer, axis, t], total)
        ref[0] = total.astype(BF)

    def rows_cols(ref):
        dims = ref.shape[1:]
        return lax.broadcasted_iota(jnp.int32, dims, 0), lax.broadcasted_iota(jnp.int32, dims, 1)

    lanes = iband_ref.shape[1] // 2
    o, n = rows_cols(iband_ref)
    toeplitz(iband_ref, 0, n % lanes, o % lanes, o // lanes == n // lanes)
    o, n = rows_cols(jband_ref)
    toeplitz(jband_ref, 1, o // SUB, n // SUB - half, o % SUB == n % SUB)
    groups = kband_ref.shape[1] // ROWS
    edge = khalo_ref.shape[1] // ROWS

    def k_of(row):
        turned = row // ROWS + jnp.where(at_end, groups - edge, 0)
        return jnp.where(turned >= groups, turned - groups, turned) * SUB + row % SUB

    def same_j(o, n):
        return (o % ROWS) // SUB == (n % ROWS) // SUB

    o, n = rows_cols(kband_ref)
    toeplitz(kband_ref, 2, k_of(o), k_of(n), same_j(o, n))
    o, n = rows_cols(khalo_ref)
    far = jnp.where(at_end, groups * SUB, -half) + (n // ROWS) * SUB + n % SUB
    toeplitz(khalo_ref, 2, k_of(o), far, same_j(o, n))


def bands(taps, lanes, j_len, kg, hg):
    layers, _, count = taps.shape
    sizes = [(2 * lanes, 2 * lanes), (j_len * SUB, (j_len + count - 1) * SUB), (kg * ROWS,) * 2, (hg * ROWS,) * 2]
    return pl.pallas_call(
        bands_kernel,
        out_shape=[shape_of(layers, *s) for s in sizes],
        grid=(layers,),
        in_specs=[pl.BlockSpec(memory_space=pltpu.SMEM)],
        out_specs=[pl.BlockSpec((1,) + s, lambda l: (l, 0, 0)) for s in sizes],
        compiler_params=pltpu.CompilerParams(dimension_semantics=("arbitrary",)),
        name='bands',
    )(taps)


def enter_kernel(vol_idx, own_ref, raw_ref, perm_ref, band_ref, vol_ref, near_ref, deep_ref, upn_ref, upd_ref, dnn_ref,
                 dnd_ref, scratch, landing, sent, landed):
    side, j_all, k_len = own_ref.shape[2], own_ref.shape[3], own_ref.shape[4]
    j_len, lanes = j_all // 2, 2 * side
    me = lax.axis_index('px')
    step, steps = pl.program_id(0), landing.shape[0]

    def to_partner(c):
        rows = pl.ds(pl.multiple_of((1 - me) * j_len, j_len), j_len)
        return pltpu.make_async_remote_copy(
            src_ref=raw_ref.at[vol_idx, pl.ds(2 * c, 2), :, rows, :], dst_ref=landing.at[c],
            send_sem=sent.at[c], recv_sem=landed.at[c],
            device_id={'px': 1 - me}, device_id_type=pl.DeviceIdType.MESH)

    @pl.when(step == 0)
    def _():
        barrier = pltpu.get_barrier_semaphore()
        pl.semaphore_signal(barrier, inc=1, device_id={'px': 1 - me}, device_id_type=pl.DeviceIdType.MESH)
        pl.semaphore_wait(barrier, 1)
        for c in range(steps):
            to_partner(c).start()

    to_partner(step).wait_recv()
    own_rows = pl.ds(pl.multiple_of(me * j_len, j_len), j_len)

    def fill(n, _):
        mine = interleave(own_ref[0, 0, n, own_rows], own_ref[0, 1, n, own_rows])
        theirs = interleave(landing[step, 0, n], landing[step, 1, n])
        for base, pair in ((me * side, mine), ((1 - me) * side, theirs)):
            scratch[pl.ds(pl.multiple_of((base + n) * PITCH, 8), j_len), :] = pair.astype(F32)
        return 0

    lax.fori_loop(0, side, fill, 0, unroll=16)
    edge_rows = near_ref.shape[1] * ROWS

    def group(g, _):
        tiles = [scratch[pl.ds(g * SUB + j, lanes, stride=PITCH), :].T.astype(BF) for j in range(SUB)]
        columns = interleave(
            jnp.concatenate([t[:k_len] for t in tiles], axis=0),
            jnp.concatenate([t[k_len:] for t in tiles], axis=0),
        )
        mixed = jnp.dot(perm_ref[...], columns, preferred_element_type=F32).astype(BF)
        filtered = jnp.dot(mixed, band_ref[...], preferred_element_type=F32).astype(BF)
        for m in range(2):
            cut = slice(m * lanes, (m + 1) * lanes)
            vol_ref[g, :, m] = mixed[:, cut].reshape(-1, ROWS, lanes)
            near_ref[g, :, m] = filtered[:edge_rows, cut].reshape(-1, ROWS, lanes)
            deep_ref[g, :, m] = filtered[edge_rows:, cut].reshape(-1, ROWS, lanes)
        return 0

    groups = j_len // SUB
    lax.fori_loop(0, groups, group, 0, unroll=8)
    hg = upn_ref.shape[0]
    upn_ref[...] = near_ref[groups - hg:]
    upd_ref[...] = deep_ref[groups - hg:]
    dnn_ref[...] = near_ref[:hg]
    dnd_ref[...] = deep_ref[:hg]

    @pl.when(step == steps - 1)
    def _():
        for c in range(steps):
            to_partner(c).wait_send()


def enter(volumes, vol_idx, perm, band, hg):
    _, chans, side, j_all, k_len = volumes.shape
    j_len = j_all // 2
    jg, kg = j_len // SUB, k_len // SUB
    steps = chans // 2
    sizes = [(jg, kg), (jg, hg), (jg, kg - hg), (hg, hg), (hg, kg - hg), (hg, hg), (hg, kg - hg)]
    return pl.pallas_call(
        functools.partial(enter_kernel, vol_idx),
        out_shape=[shape_of(*s, chans, ROWS, 2 * side) for s in sizes],
        grid=(steps,),
        in_specs=[
            pl.BlockSpec((1, 2, side, j_all, k_len), lambda c: (vol_idx, c, 0, 0, 0)),
            pl.BlockSpec(memory_space=pl.ANY),
            pl.BlockSpec(perm.shape, lambda c: (0, 0)),
            pl.BlockSpec((None,) + band.shape[1:], lambda c: (0, 0, 0)),
        ],
        out_specs=[pl.BlockSpec(s + (2, ROWS, 2 * side), lambda c: (0, 0, c, 0, 0)) for s in sizes],
        scratch_shapes=[
            pltpu.VMEM((2 * side * PITCH, 2 * k_len), F32),
            pltpu.VMEM((steps, 2, side, j_len, k_len), BF),
            pltpu.SemaphoreType.DMA((steps,)),
            pltpu.SemaphoreType.DMA((steps,)),
        ],
        compiler_params=pltpu.CompilerParams(
            dimension_semantics=("arbitrary",), collective_id=vol_idx, has_side_effects=True),
        cost_estimate=pl.CostEstimate(flops=chans * 1_000_000_000, bytes_accessed=chans * 2_500_000, transcendentals=0),
    )(volumes, volumes, perm, band)


def leave_kernel(half_ref, own_ref, other_ref, perm_ref, *refs):
    raw_ref, scratch = refs[-2:]
    side, j_all, k_len = raw_ref.shape[2], raw_ref.shape[3], raw_ref.shape[4]
    lanes = own_ref.shape[4]
    j_len = j_all // 2
    half = half_ref[0]
    left = lax.broadcasted_iota(jnp.int32, (own_ref.shape[1] * ROWS, lanes), 1) < side

    def group(g, _):
        chan = []
        for m in range(2):
            a, b = own_ref[g, :, m].reshape(-1, lanes), other_ref[g, :, m].reshape(-1, lanes)
            chan.append(jnp.concatenate([
                interleave(a[:, :side], b[:, :side]), interleave(a[:, side:], b[:, side:])], axis=0))
        rows = jnp.dot(perm_ref[...], interleave(*chan), preferred_element_type=F32)
        for j in range(SUB):
            part = rows[j * k_len:(j + 1) * k_len]
            tile = jnp.concatenate([part[:, :lanes], part[:, lanes:]], axis=0)
            scratch[pl.ds(g * SUB + j, lanes, stride=PITCH), :] = tile.T
        return 0

    lax.fori_loop(0, j_len // SUB, group, 0, unroll=8)

    def drain(n, _):
        for base, where in ((0, half), (side, 1 - half)):
            pair = scratch[pl.ds(pl.multiple_of((base + n) * PITCH, 8), j_len), :].astype(BF)
            at = pl.ds(pl.multiple_of(where * j_len, j_len), j_len)
            raw_ref[0, 0, n, at] = pair[:, :k_len]
            raw_ref[0, 1, n, at] = pair[:, k_len:]
        return 0

    lax.fori_loop(0, side, drain, 0, unroll=16)


def leave(own, other, vol_idx, result, half, perm, full_shape):
    _, chans, side, j_all, k_len = full_shape
    jg, kp = own.shape[:2]
    operands = [half, own, other, perm]
    spec = pl.BlockSpec((jg, kp, 2, ROWS, 2 * side), lambda c, h: (0, 0, c, 0, 0))
    in_specs = [spec, spec, pl.BlockSpec(perm.shape, lambda c, h: (0, 0))]
    aliases = {}
    if result is not None:
        operands.append(result)
        in_specs.append(pl.BlockSpec(memory_space=pl.ANY))
        aliases = {4: 0}
    return pl.pallas_call(
        leave_kernel,
        out_shape=shape_of(*full_shape),
        grid_spec=pltpu.PrefetchScalarGridSpec(
            num_scalar_prefetch=1,
            grid=(chans // 2,),
            in_specs=in_specs,
            out_specs=pl.BlockSpec((1, 2, side, j_all, k_len), lambda c, h: (vol_idx, c, 0, 0, 0)),
            scratch_shapes=[pltpu.VMEM((2 * side * PITCH, 2 * k_len), F32)],
        ),
        input_output_aliases=aliases,
        compiler_params=pltpu.CompilerParams(dimension_semantics=("arbitrary",)),
        cost_estimate=pl.CostEstimate(flops=30_000_000_000, bytes_accessed=50_000_000, transcendentals=0),
    )(*operands)


def along_j_kernel(field_ref, low_ref, high_ref, band_ref, out_ref):
    count, chans, lanes = field_ref.shape[1], field_ref.shape[2], field_ref.shape[4]

    def group(k, _):
        for first in range(0, chans, 2):
            halves = [jnp.concatenate([ref[:, k, c].reshape(-1, lanes) for ref in (low_ref, field_ref, high_ref)], axis=0)
                      for c in (first, first + 1)]
            total = jnp.dot(band_ref[...], interleave(*halves), preferred_element_type=F32).astype(BF)
            for m in range(2):
                out_ref[:, k, first + m] = total[:, m * lanes:(m + 1) * lanes].reshape(-1, ROWS, lanes)
        return 0

    lax.fori_loop(0, count, group, 0)


def along_j(field, low, high, band, layer):
    _, count, chans, rows, lanes = field.shape
    width = CHAN_STEP
    block = lambda a: pl.BlockSpec((a.shape[0], count, width, rows, lanes), lambda c: (0, 0, c, 0, 0))
    return pl.pallas_call(
        along_j_kernel,
        out_shape=shape_of(*field.shape),
        grid=(chans // width,),
        in_specs=[block(field), block(low), block(high), pl.BlockSpec((None,) + band.shape[1:], lambda c: (layer, 0, 0))],
        out_specs=block(field),
        compiler_params=pltpu.CompilerParams(dimension_semantics=("arbitrary",)),
        cost_estimate=pl.CostEstimate(flops=count * 1_000_000_000, bytes_accessed=count * 2_900_000, transcendentals=0),
    )(field, low, high, band)


GELU_A = 0.7978845608028654
GELU_B = GELU_A * 0.044715


def finish_kernel(last, edge_ref, rest_ref, halo_ref, vol_ref, band_ref, halo_band_ref, mix_ref, bias_ref, *refs):
    unit = refs[-1]
    edge = edge_ref.shape[1]
    groups, chans, lanes = vol_ref.shape[1], vol_ref.shape[2], vol_ref.shape[4]
    edge_rows = edge * ROWS

    def channel_pair(n, _):
        own, far = [], []
        for m in range(2):
            c = 2 * n + m
            own.append(jnp.concatenate(
                [edge_ref[0, :, c].reshape(-1, lanes), rest_ref[0, :, c].reshape(-1, lanes)], axis=0))
            far.append(halo_ref[0, :, c].reshape(-1, lanes))
        total = jnp.dot(band_ref[...], interleave(*own), preferred_element_type=F32)
        extra = jnp.dot(halo_band_ref[...], interleave(*far), preferred_element_type=F32)
        head = (total[:edge_rows] + extra).astype(BF)
        tail = total[edge_rows:].astype(BF)
        for m in range(2):
            cut = slice(m * lanes, (m + 1) * lanes)
            unit[:edge, 2 * n + m] = head[:, cut].reshape(-1, ROWS, lanes)
            unit[edge:, 2 * n + m] = tail[:, cut].reshape(-1, ROWS, lanes)
        return 0

    lax.fori_loop(0, chans // 2, channel_pair, 0, unroll=chans // 2)

    def group_pair(n, _):
        k0, k1 = (n, n + groups // 2) if last else (2 * n, 2 * n + 1)
        both = lambda ref, lead: interleave(
            ref[lead + (k0,)].reshape(-1, lanes), ref[lead + (k1,)].reshape(-1, lanes))
        x = jnp.dot(mix_ref[...], both(unit, ()), preferred_element_type=F32) + interleave(bias_ref[...], bias_ref[...])
        half_x = 0.5 * x
        act = half_x * jnp.tanh(x * (GELU_A + GELU_B * (x * x))) + half_x
        new = (both(vol_ref, (0,)).astype(F32) + act).astype(BF)
        shaped = lambda a: a.reshape(chans, ROWS, lanes)
        if last:
            own_ref, other_ref = refs[:2]
            side = lanes // 2
            low = interleave(new[:, :side], new[:, lanes:lanes + side])
            high = interleave(new[:, side:lanes], new[:, lanes + side:])
            is_low = lax.axis_index('px') == 0
            own_ref[0, n] = shaped(jnp.where(is_low, low, high))
            other_ref[0, n] = shaped(jnp.where(is_low, high, low))
        else:
            new_ref = refs[1]
            new_ref[0, k0], new_ref[0, k1] = shaped(new[:, :lanes]), shaped(new[:, lanes:])
        return 0

    lax.fori_loop(0, groups // 2, group_pair, 0, unroll=4)

    if not last:
        iband_ref, new_ref, near_ref, deep_ref, upn_ref, upd_ref, dnn_ref, dnd_ref = refs[:8]
        g = pl.program_id(0)
        many = groups // 2

        for first in range(0, groups, many):
            pairs = [interleave(new_ref[0, first + q].reshape(-1, lanes), new_ref[0, first + many // 2 + q].reshape(-1, lanes))
                     for q in range(many // 2)]
            filt = jnp.dot(jnp.concatenate(pairs, axis=0), iband_ref[...], preferred_element_type=F32).astype(BF)
            for m in range(2):
                groups_of = filt[:, m * lanes:(m + 1) * lanes].reshape(many // 2, chans, ROWS, lanes)
                at = first + m * (many // 2)
                cut = min(max(edge - at, 0), many // 2)
                if cut > 0:
                    near_ref[0, at:at + cut] = groups_of[:cut]
                if cut < many // 2:
                    deep_ref[0, at + cut - edge:at + many // 2 - edge] = groups_of[cut:]

        @pl.when(g < edge)
        def _():
            dnn_ref[0] = near_ref[0]
            dnd_ref[0] = deep_ref[0]

        @pl.when(g >= pl.num_programs(0) - edge)
        def _():
            upn_ref[0] = near_ref[0]
            upd_ref[0] = deep_ref[0]


def finish(edge, rest, halo, vol, layer, band, halo_band, mix, bias, iband):
    jg, kg, chans, rows, lanes = vol.shape
    hg = edge.shape[1]
    last = iband is None
    block = lambda a: pl.BlockSpec((1,) + a.shape[1:], lambda g: (g, 0, 0, 0, 0))
    of_layer = lambda a, l: pl.BlockSpec((None,) + a.shape[1:], lambda g: (l, 0, 0))
    in_specs = [block(edge), block(rest), block(halo), block(vol)]
    in_specs += [of_layer(a, layer) for a in (band, halo_band, mix, bias)]
    operands = [edge, rest, halo, vol, band, halo_band, mix, bias]
    if last:
        packed = shape_of(jg, kg // 2, chans, rows, lanes)
        out_shape, out_specs = [packed] * 2, [block(packed)] * 2
    else:
        operands.append(iband)
        in_specs.append(of_layer(iband, layer + 1))
        out_shape = [shape_of(*vol.shape), shape_of(*edge.shape), shape_of(*rest.shape)]
        out_specs = [block(vol), block(edge), block(rest)]
        up = lambda g: (jnp.maximum(g - (jg - hg), 0), 0, 0, 0, 0)
        down = lambda g: (jnp.minimum(g, hg - 1), 0, 0, 0, 0)
        for index in (up, down):
            for size in (hg, kg - hg):
                out_shape.append(shape_of(hg, size, chans, rows, lanes))
                out_specs.append(pl.BlockSpec((1, size, chans, rows, lanes), index))
    return pl.pallas_call(
        functools.partial(finish_kernel, last),
        out_shape=out_shape,
        grid=(jg,),
        in_specs=in_specs,
        out_specs=out_specs,
        scratch_shapes=[pltpu.VMEM((kg, chans, rows, lanes), BF)],
        compiler_params=pltpu.CompilerParams(dimension_semantics=("arbitrary",)),
        cost_estimate=pl.CostEstimate(flops=40_000_000_000, bytes_accessed=75_000_000, transcendentals=8_400_000),
    )(*operands)


def solution(mesh):
    sizes = {a: mesh.shape[a] for a in ('px', 'py', 'pz')}
    vol_spec = P('dp', None, 'px', 'py', 'pz')

    def local_layers(volumes, filter_taps, mix_weight, mix_bias):
        count, chans, side, j_all, k_len = volumes.shape
        layers, _, taps = filter_taps.shape
        half = (taps - 1) // 2
        j_len = j_all // 2
        kg, hg = k_len // SUB, half // SUB
        px, pz = lax.axis_index('px'), lax.axis_index('pz')
        half_idx = px.astype(jnp.int32).reshape(1)
        iband, jband, kband, khalo = bands(filter_taps.astype(BF).astype(F32), 2 * side, j_len, kg, hg)

        o, n = grid2(chans * ROWS, chans * ROWS)
        spread = jnp.repeat(jnp.repeat(mix_weight.swapaxes(1, 2), ROWS, axis=1), ROWS, axis=2)
        mix = jnp.where(o % ROWS == n % ROWS, spread, jnp.zeros((), BF))
        bias = jnp.broadcast_to(jnp.repeat(mix_bias, ROWS, axis=1)[:, :, None], (layers, chans * ROWS, 2 * side))

        o, n = grid2(kg * ROWS, SUB * k_len)
        k_row = jnp.where(pz == 0, (o // ROWS + kg - hg) % kg, o // ROWS) * SUB + o % SUB
        perm = jnp.where(n == ((o % ROWS) // SUB) * k_len + k_row, 1.0, 0.0).astype(BF)

        swap = [(0, 1), (1, 0)]
        line = sizes['py'] * sizes['px']
        upward = [(s, s + 1) for s in range(line - 1)]
        downward = [(s + 1, s) for s in range(line - 1)]
        up = lambda a: lax.ppermute(a, ('py', 'px'), upward)
        down = lambda a: lax.ppermute(a, ('py', 'px'), downward)

        states = []
        for v in range(count):
            states.append(enter(volumes, v, perm, iband, hg))
        result = None

        def send_j(v):
            up_near, up_deep, down_near, down_deep = states[v][3:]
            moved = []
            for move, part in ((up, up_near), (down, down_near),
                                     (up, up_deep), (down, down_deep)):
                moved.append(move(part))
            return moved

        def edge_of(l, v, after):
            filt = states[v][1]
            if after is not None:
                filt, after = lax.optimization_barrier((filt, after))
            edge = along_j(filt, *halos[v][:2], jband, l)
            return edge, lax.ppermute(edge, 'pz', swap), after

        halos = [send_j(v) for v in range(count)]
        edges = [edge_of(0, 0, None)] + [None] * (count - 1)
        rests = [None] * count
        rests[0] = along_j(states[0][2], *halos[0][2:], jband, 0)
        for step in range(count * layers):
            l, v = divmod(step, count)
            nl, nv = divmod(step + 1, count)
            if nl < layers and edges[nv] is None:
                edges[nv] = edge_of(nl, nv, rests[v])
                rests[v] = edges[nv][2]
            edge, halo, _ = edges[v]
            states[v] = finish(edge, rests[v], halo, states[v][0], l, kband, khalo, mix, bias,
                               iband if l + 1 < layers else None)
            edges[v] = rests[v] = None
            if l + 1 < layers:
                halos[v] = send_j(v)
            if nl < layers:
                rests[nv] = along_j(states[nv][2], *halos[nv][2:], jband, nl)
        for v in range(count):
            own, other = states[v]
            other = lax.ppermute(other, 'px', swap)
            result = leave(own, other, v, result, half_idx, perm.T, volumes.shape)
        return result

    return jax.shard_map(local_layers, mesh=mesh, in_specs=(vol_spec, P(), P(), P()), out_specs=vol_spec, check_vma=False)
```

```python
import functools

import jax
import jax.numpy as jnp
from jax import lax
from jax.experimental import pallas as pl
from jax.experimental.pallas import tpu as pltpu
from jax.sharding import PartitionSpec as P


BF = jnp.bfloat16
F32 = jnp.float32
SUB = 4
ROWS = SUB * SUB
PITCH = 40
CHAN_STEP = 8


def shape_of(*dims, dtype=BF):
    return jax.ShapeDtypeStruct(dims, dtype)


def grid2(rows, cols):
    return lax.broadcasted_iota(jnp.int32, (rows, cols), 0), lax.broadcasted_iota(jnp.int32, (rows, cols), 1)


def interleave(first, second):
    return jnp.concatenate([first, second], axis=1)


def bands_kernel(taps_ref, iband_ref, jband_ref, kband_ref, khalo_ref):
    layer = pl.program_id(0)
    at_end = lax.axis_index('pz') == 0
    half = (taps_ref.shape[2] - 1) // 2

    def toeplitz(ref, axis, out_pos, in_pos, keep):
        tap = jnp.where(keep, in_pos - out_pos + half, -1)
        total = jnp.zeros(tap.shape, F32)
        for t in range(2 * half + 1):
            total = jnp.where(tap == t, taps_ref[layer, axis, t], total)
        ref[0] = total.astype(BF)

    def rows_cols(ref):
        dims = ref.shape[1:]
        return lax.broadcasted_iota(jnp.int32, dims, 0), lax.broadcasted_iota(jnp.int32, dims, 1)

    lanes = iband_ref.shape[1] // 2
    o, n = rows_cols(iband_ref)
    toeplitz(iband_ref, 0, n % lanes, o % lanes, o // lanes == n // lanes)
    o, n = rows_cols(jband_ref)
    toeplitz(jband_ref, 1, o // SUB, n // SUB - half, o % SUB == n % SUB)
    groups = kband_ref.shape[1] // ROWS
    edge = khalo_ref.shape[1] // ROWS

    def k_of(row):
        turned = row // ROWS + jnp.where(at_end, groups - edge, 0)
        return jnp.where(turned >= groups, turned - groups, turned) * SUB + row % SUB

    def same_j(o, n):
        return (o % ROWS) // SUB == (n % ROWS) // SUB

    o, n = rows_cols(kband_ref)
    toeplitz(kband_ref, 2, k_of(o), k_of(n), same_j(o, n))
    o, n = rows_cols(khalo_ref)
    far = jnp.where(at_end, groups * SUB, -half) + (n // ROWS) * SUB + n % SUB
    toeplitz(khalo_ref, 2, k_of(o), far, same_j(o, n))


def bands(taps, lanes, j_len, kg, hg):
    layers, _, count = taps.shape
    sizes = [(2 * lanes, 2 * lanes), (j_len * SUB, (j_len + count - 1) * SUB), (kg * ROWS,) * 2, (hg * ROWS,) * 2]
    return pl.pallas_call(
        bands_kernel,
        out_shape=[shape_of(layers, *s) for s in sizes],
        grid=(layers,),
        in_specs=[pl.BlockSpec(memory_space=pltpu.SMEM)],
        out_specs=[pl.BlockSpec((1,) + s, lambda l: (l, 0, 0)) for s in sizes],
        compiler_params=pltpu.CompilerParams(dimension_semantics=("arbitrary",)),
        name='bands',
    )(taps)


def enter_kernel(vol_idx, own_ref, raw_ref, perm_ref, band_ref, vol_ref, near_ref, deep_ref, upn_ref, upd_ref, dnn_ref,
                 dnd_ref, scratch, landing, sent, landed):
    side, j_len, k_len = own_ref.shape[2], own_ref.shape[3], own_ref.shape[4]
    lanes = 2 * side
    me = lax.axis_index('px')
    step, steps = pl.program_id(0), landing.shape[0]

    def to_partner(c):
        rows = pl.ds(pl.multiple_of((1 - me) * j_len, j_len), j_len)
        return pltpu.make_async_remote_copy(
            src_ref=raw_ref.at[vol_idx, pl.ds(2 * c, 2), :, rows, :], dst_ref=landing.at[c],
            send_sem=sent.at[c], recv_sem=landed.at[c],
            device_id={'px': 1 - me}, device_id_type=pl.DeviceIdType.MESH)

    @pl.when(step == 0)
    def _():
        barrier = pltpu.get_barrier_semaphore()
        pl.semaphore_signal(barrier, inc=1, device_id={'px': 1 - me}, device_id_type=pl.DeviceIdType.MESH)
        pl.semaphore_wait(barrier, 1)
        for c in range(steps):
            to_partner(c).start()

    to_partner(step).wait_recv()

    def fill(n, _):
        mine = interleave(own_ref[0, 0, n], own_ref[0, 1, n])
        theirs = interleave(landing[step, 0, n], landing[step, 1, n])
        for base, pair in ((me * side, mine), ((1 - me) * side, theirs)):
            scratch[pl.ds(pl.multiple_of((base + n) * PITCH, 8), j_len), :] = pair.astype(F32)
        return 0

    lax.fori_loop(0, side, fill, 0, unroll=16)
    edge_rows = near_ref.shape[1] * ROWS

    def group(g, _):
        tiles = [scratch[pl.ds(g * SUB + j, lanes, stride=PITCH), :].T.astype(BF) for j in range(SUB)]
        columns = interleave(
            jnp.concatenate([t[:k_len] for t in tiles], axis=0),
            jnp.concatenate([t[k_len:] for t in tiles], axis=0),
        )
        mixed = jnp.dot(perm_ref[...], columns, preferred_element_type=F32).astype(BF)
        filtered = jnp.dot(mixed, band_ref[...], preferred_element_type=F32).astype(BF)
        for m in range(2):
            cut = slice(m * lanes, (m + 1) * lanes)
            vol_ref[g, :, m] = mixed[:, cut].reshape(-1, ROWS, lanes)
            near_ref[g, :, m] = filtered[:edge_rows, cut].reshape(-1, ROWS, lanes)
            deep_ref[g, :, m] = filtered[edge_rows:, cut].reshape(-1, ROWS, lanes)
        return 0

    groups = j_len // SUB
    lax.fori_loop(0, groups, group, 0, unroll=8)
    hg = upn_ref.shape[0]
    upn_ref[...] = near_ref[groups - hg:]
    upd_ref[...] = deep_ref[groups - hg:]
    dnn_ref[...] = near_ref[:hg]
    dnd_ref[...] = deep_ref[:hg]

    @pl.when(step == steps - 1)
    def _():
        for c in range(steps):
            to_partner(c).wait_send()


def enter(volumes, vol_idx, perm, band, hg):
    _, chans, side, j_all, k_len = volumes.shape
    j_len = j_all // 2
    jg, kg = j_len // SUB, k_len // SUB
    steps = chans // 2
    sizes = [(jg, kg), (jg, hg), (jg, kg - hg), (hg, hg), (hg, kg - hg), (hg, hg), (hg, kg - hg)]
    return pl.pallas_call(
        functools.partial(enter_kernel, vol_idx),
        out_shape=[shape_of(*s, chans, ROWS, 2 * side) for s in sizes],
        grid=(steps,),
        in_specs=[
            pl.BlockSpec((1, 2, side, j_len, k_len), lambda c: (vol_idx, c, 0, lax.axis_index('px'), 0)),
            pl.BlockSpec(memory_space=pl.ANY),
            pl.BlockSpec(perm.shape, lambda c: (0, 0)),
            pl.BlockSpec((None,) + band.shape[1:], lambda c: (0, 0, 0)),
        ],
        out_specs=[pl.BlockSpec(s + (2, ROWS, 2 * side), lambda c: (0, 0, c, 0, 0)) for s in sizes],
        scratch_shapes=[
            pltpu.VMEM((2 * side * PITCH, 2 * k_len), F32),
            pltpu.VMEM((steps, 2, side, j_len, k_len), BF),
            pltpu.SemaphoreType.DMA((steps,)),
            pltpu.SemaphoreType.DMA((steps,)),
        ],
        compiler_params=pltpu.CompilerParams(
            dimension_semantics=("arbitrary",), collective_id=vol_idx, has_side_effects=True),
        cost_estimate=pl.CostEstimate(flops=chans * 1_000_000_000, bytes_accessed=chans * 2_500_000, transcendentals=0),
    )(volumes, volumes, perm, band)


def leave_kernel(half_ref, own_ref, other_ref, perm_ref, *refs):
    raw_ref, scratch = refs[-2:]
    side, j_all, k_len = raw_ref.shape[2], raw_ref.shape[3], raw_ref.shape[4]
    lanes = own_ref.shape[4]
    j_len = j_all // 2
    half = half_ref[0]
    left = lax.broadcasted_iota(jnp.int32, (own_ref.shape[1] * ROWS, lanes), 1) < side

    def group(g, _):
        chan = []
        for m in range(2):
            a, b = own_ref[g, :, m].reshape(-1, lanes), other_ref[g, :, m].reshape(-1, lanes)
            chan.append(jnp.concatenate([
                interleave(a[:, :side], b[:, :side]), interleave(a[:, side:], b[:, side:])], axis=0))
        rows = jnp.dot(perm_ref[...], interleave(*chan), preferred_element_type=F32)
        for j in range(SUB):
            part = rows[j * k_len:(j + 1) * k_len]
            tile = jnp.concatenate([part[:, :lanes], part[:, lanes:]], axis=0)
            scratch[pl.ds(g * SUB + j, lanes, stride=PITCH), :] = tile.T
        return 0

    lax.fori_loop(0, j_len // SUB, group, 0, unroll=8)

    def drain(n, _):
        for base, where in ((0, half), (side, 1 - half)):
            pair = scratch[pl.ds(pl.multiple_of((base + n) * PITCH, 8), j_len), :].astype(BF)
            at = pl.ds(pl.multiple_of(where * j_len, j_len), j_len)
            raw_ref[0, 0, n, at] = pair[:, :k_len]
            raw_ref[0, 1, n, at] = pair[:, k_len:]
        return 0

    lax.fori_loop(0, side, drain, 0, unroll=32)


def leave(own, other, vol_idx, result, half, perm, full_shape):
    _, chans, side, j_all, k_len = full_shape
    jg, kp = own.shape[:2]
    operands = [half, own, other, perm]
    spec = pl.BlockSpec((jg, kp, 2, ROWS, 2 * side), lambda c, h: (0, 0, c, 0, 0))
    in_specs = [spec, spec, pl.BlockSpec(perm.shape, lambda c, h: (0, 0))]
    aliases = {}
    if result is not None:
        operands.append(result)
        in_specs.append(pl.BlockSpec(memory_space=pl.ANY))
        aliases = {4: 0}
    return pl.pallas_call(
        leave_kernel,
        out_shape=shape_of(*full_shape),
        grid_spec=pltpu.PrefetchScalarGridSpec(
            num_scalar_prefetch=1,
            grid=(chans // 2,),
            in_specs=in_specs,
            out_specs=pl.BlockSpec((1, 2, side, j_all, k_len), lambda c, h: (vol_idx, c, 0, 0, 0)),
            scratch_shapes=[pltpu.VMEM((2 * side * PITCH, 2 * k_len), F32)],
        ),
        input_output_aliases=aliases,
        compiler_params=pltpu.CompilerParams(dimension_semantics=("arbitrary",)),
        cost_estimate=pl.CostEstimate(flops=30_000_000_000, bytes_accessed=50_000_000, transcendentals=0),
    )(*operands)


def along_j_kernel(field_ref, low_ref, high_ref, band_ref, out_ref):
    count, chans, lanes = field_ref.shape[1], field_ref.shape[2], field_ref.shape[4]

    def group(k, _):
        for first in range(0, chans, 2):
            halves = [jnp.concatenate([ref[:, k, c].reshape(-1, lanes) for ref in (low_ref, field_ref, high_ref)], axis=0)
                      for c in (first, first + 1)]
            total = jnp.dot(band_ref[...], interleave(*halves), preferred_element_type=F32).astype(BF)
            for m in range(2):
                out_ref[:, k, first + m] = total[:, m * lanes:(m + 1) * lanes].reshape(-1, ROWS, lanes)
        return 0

    lax.fori_loop(0, count, group, 0, unroll=count if count > low_ref.shape[0] else 1)


def along_j(field, low, high, band, layer):
    _, count, chans, rows, lanes = field.shape
    width = CHAN_STEP
    block = lambda a: pl.BlockSpec((a.shape[0], count, width, rows, lanes), lambda c: (0, 0, c, 0, 0))
    return pl.pallas_call(
        along_j_kernel,
        out_shape=shape_of(*field.shape),
        grid=(chans // width,),
        in_specs=[block(field), block(low), block(high), pl.BlockSpec((None,) + band.shape[1:], lambda c: (layer, 0, 0))],
        out_specs=block(field),
        compiler_params=pltpu.CompilerParams(dimension_semantics=("arbitrary",)),
        cost_estimate=pl.CostEstimate(flops=count * 1_000_000_000, bytes_accessed=count * 2_900_000, transcendentals=0),
    )(field, low, high, band)


GELU_A = 0.7978845608028654
GELU_B = GELU_A * 0.044715


def finish_kernel(last, edge_ref, rest_ref, halo_ref, vol_ref, band_ref, halo_band_ref, mix_ref, bias_ref, *refs):
    unit = refs[-1]
    edge = edge_ref.shape[1]
    groups, chans, lanes = vol_ref.shape[1], vol_ref.shape[2], vol_ref.shape[4]
    edge_rows = edge * ROWS

    def channel_pair(n, _):
        own, far = [], []
        for m in range(2):
            c = 2 * n + m
            own.append(jnp.concatenate(
                [edge_ref[0, :, c].reshape(-1, lanes), rest_ref[0, :, c].reshape(-1, lanes)], axis=0))
            far.append(halo_ref[0, :, c].reshape(-1, lanes))
        total = jnp.dot(band_ref[...], interleave(*own), preferred_element_type=F32)
        extra = jnp.dot(halo_band_ref[...], interleave(*far), preferred_element_type=F32)
        head = (total[:edge_rows] + extra).astype(BF)
        tail = total[edge_rows:].astype(BF)
        for m in range(2):
            cut = slice(m * lanes, (m + 1) * lanes)
            unit[:edge, 2 * n + m] = head[:, cut].reshape(-1, ROWS, lanes)
            unit[edge:, 2 * n + m] = tail[:, cut].reshape(-1, ROWS, lanes)
        return 0

    lax.fori_loop(0, chans // 2, channel_pair, 0, unroll=chans // 2)

    def group_pair(n, _):
        k0, k1 = (n, n + groups // 2) if last else (2 * n, 2 * n + 1)
        both = lambda ref, lead: interleave(
            ref[lead + (k0,)].reshape(-1, lanes), ref[lead + (k1,)].reshape(-1, lanes))
        x = jnp.dot(mix_ref[...], both(unit, ()), preferred_element_type=F32) + interleave(bias_ref[...], bias_ref[...])
        half_x = 0.5 * x
        act = half_x * jnp.tanh(x * (GELU_A + GELU_B * (x * x))) + half_x
        new = (both(vol_ref, (0,)).astype(F32) + act).astype(BF)
        shaped = lambda a: a.reshape(chans, ROWS, lanes)
        if last:
            own_ref, other_ref = refs[:2]
            side = lanes // 2
            low = interleave(new[:, :side], new[:, lanes:lanes + side])
            high = interleave(new[:, side:lanes], new[:, lanes + side:])
            is_low = lax.axis_index('px') == 0
            own_ref[0, n] = shaped(jnp.where(is_low, low, high))
            other_ref[0, n] = shaped(jnp.where(is_low, high, low))
        else:
            new_ref = refs[1]
            new_ref[0, k0], new_ref[0, k1] = shaped(new[:, :lanes]), shaped(new[:, lanes:])
        return 0

    lax.fori_loop(0, groups // 2, group_pair, 0, unroll=8)

    if not last:
        iband_ref, new_ref, near_ref, deep_ref, upn_ref, upd_ref, dnn_ref, dnd_ref = refs[:8]
        g = pl.program_id(0)
        many = groups // 2

        for first in range(0, groups, many):
            pairs = [interleave(new_ref[0, first + q].reshape(-1, lanes), new_ref[0, first + many // 2 + q].reshape(-1, lanes))
                     for q in range(many // 2)]
            filt = jnp.dot(jnp.concatenate(pairs, axis=0), iband_ref[...], preferred_element_type=F32).astype(BF)
            for m in range(2):
                groups_of = filt[:, m * lanes:(m + 1) * lanes].reshape(many // 2, chans, ROWS, lanes)
                at = first + m * (many // 2)
                cut = min(max(edge - at, 0), many // 2)
                if cut > 0:
                    near_ref[0, at:at + cut] = groups_of[:cut]
                if cut < many // 2:
                    deep_ref[0, at + cut - edge:at + many // 2 - edge] = groups_of[cut:]

        @pl.when(g < edge)
        def _():
            dnn_ref[0] = near_ref[0]
            dnd_ref[0] = deep_ref[0]

        @pl.when(g >= pl.num_programs(0) - edge)
        def _():
            upn_ref[0] = near_ref[0]
            upd_ref[0] = deep_ref[0]


def finish(edge, rest, halo, vol, layer, band, halo_band, mix, bias, iband):
    jg, kg, chans, rows, lanes = vol.shape
    hg = edge.shape[1]
    last = iband is None
    block = lambda a: pl.BlockSpec((1,) + a.shape[1:], lambda g: (g, 0, 0, 0, 0))
    of_layer = lambda a, l: pl.BlockSpec((None,) + a.shape[1:], lambda g: (l, 0, 0))
    in_specs = [block(edge), block(rest), block(halo), block(vol)]
    in_specs += [of_layer(a, layer) for a in (band, halo_band, mix, bias)]
    operands = [edge, rest, halo, vol, band, halo_band, mix, bias]
    if last:
        packed = shape_of(jg, kg // 2, chans, rows, lanes)
        out_shape, out_specs = [packed] * 2, [block(packed)] * 2
    else:
        operands.append(iband)
        in_specs.append(of_layer(iband, layer + 1))
        out_shape = [shape_of(*vol.shape), shape_of(*edge.shape), shape_of(*rest.shape)]
        out_specs = [block(vol), block(edge), block(rest)]
        up = lambda g: (jnp.maximum(g - (jg - hg), 0), 0, 0, 0, 0)
        down = lambda g: (jnp.minimum(g, hg - 1), 0, 0, 0, 0)
        for index in (up, down):
            for size in (hg, kg - hg):
                out_shape.append(shape_of(hg, size, chans, rows, lanes))
                out_specs.append(pl.BlockSpec((1, size, chans, rows, lanes), index))
    return pl.pallas_call(
        functools.partial(finish_kernel, last),
        out_shape=out_shape,
        grid=(jg,),
        in_specs=in_specs,
        out_specs=out_specs,
        scratch_shapes=[pltpu.VMEM((kg, chans, rows, lanes), BF)],
        compiler_params=pltpu.CompilerParams(dimension_semantics=("arbitrary",)),
        cost_estimate=pl.CostEstimate(flops=40_000_000_000, bytes_accessed=75_000_000, transcendentals=8_400_000),
    )(*operands)


def solution(mesh):
    sizes = {a: mesh.shape[a] for a in ('px', 'py', 'pz')}
    vol_spec = P('dp', None, 'px', 'py', 'pz')

    def local_layers(volumes, filter_taps, mix_weight, mix_bias):
        count, chans, side, j_all, k_len = volumes.shape
        layers, _, taps = filter_taps.shape
        half = (taps - 1) // 2
        j_len = j_all // 2
        kg, hg = k_len // SUB, half // SUB
        px, pz = lax.axis_index('px'), lax.axis_index('pz')
        half_idx = px.astype(jnp.int32).reshape(1)
        iband, jband, kband, khalo = bands(filter_taps.astype(BF).astype(F32), 2 * side, j_len, kg, hg)

        o, n = grid2(chans * ROWS, chans * ROWS)
        spread = jnp.repeat(jnp.repeat(mix_weight.swapaxes(1, 2), ROWS, axis=1), ROWS, axis=2)
        mix = jnp.where(o % ROWS == n % ROWS, spread, jnp.zeros((), BF))
        bias = jnp.broadcast_to(jnp.repeat(mix_bias, ROWS, axis=1)[:, :, None], (layers, chans * ROWS, 2 * side))

        o, n = grid2(kg * ROWS, SUB * k_len)
        k_row = jnp.where(pz == 0, (o // ROWS + kg - hg) % kg, o // ROWS) * SUB + o % SUB
        perm = jnp.where(n == ((o % ROWS) // SUB) * k_len + k_row, 1.0, 0.0).astype(BF)

        swap = [(0, 1), (1, 0)]
        line = sizes['py'] * sizes['px']
        upward = [(s, s + 1) for s in range(line - 1)]
        downward = [(s + 1, s) for s in range(line - 1)]
        up = lambda a: lax.ppermute(a, ('py', 'px'), upward)
        down = lambda a: lax.ppermute(a, ('py', 'px'), downward)

        states = []
        for v in range(count):
            states.append(enter(volumes, v, perm, iband, hg))
        result = None

        def send_j(v):
            up_near, up_deep, down_near, down_deep = states[v][3:]
            moved = []
            for move, part in ((up, up_near), (down, down_near),
                                     (up, up_deep), (down, down_deep)):
                moved.append(move(part))
            return moved

        def edge_of(l, v, after):
            filt = states[v][1]
            if after is not None:
                filt, after = lax.optimization_barrier((filt, after))
            edge = along_j(filt, *halos[v][:2], jband, l)
            return edge, lax.ppermute(edge, 'pz', swap), after

        halos = [send_j(v) for v in range(count)]
        edges = [edge_of(0, 0, None)] + [None] * (count - 1)
        rests = [None] * count
        rests[0] = along_j(states[0][2], *halos[0][2:], jband, 0)
        for step in range(count * layers):
            l, v = divmod(step, count)
            nl, nv = divmod(step + 1, count)
            if nl < layers and edges[nv] is None:
                edges[nv] = edge_of(nl, nv, rests[v])
                rests[v] = edges[nv][2]
            edge, halo, _ = edges[v]
            states[v] = finish(edge, rests[v], halo, states[v][0], l, kband, khalo, mix, bias,
                               iband if l + 1 < layers else None)
            edges[v] = rests[v] = None
            if l + 1 < layers:
                halos[v] = send_j(v)
            if nl < layers:
                rests[nv] = along_j(states[nv][2], *halos[nv][2:], jband, nl)
        for v in range(count):
            own, other = states[v]
            other = lax.ppermute(other, 'px', swap)
            result = leave(own, other, v, result, half_idx, perm.T, volumes.shape)
        return result

    return jax.shard_map(local_layers, mesh=mesh, in_specs=(vol_spec, P(), P(), P()), out_specs=vol_spec, check_vma=False)
```
